512 devices in a mesh: row: 16 (over x_hi, y, core), col: 32 (over z, x_lo).
Axes of the slice: x: 4 (x_hi: 2, x_lo: 2; x = x_hi * 2 + x_lo), y: 4, z: 16, core: 2. Of those that a mesh axis runs over, the one named last changes fastest.
Arguments:
- tokens: bfloat16 [256, 16384], P('row', 'col'), may hold values from -6 to 6
- gate_weight: bfloat16 [16384, 26624], P('col', 'row'), may hold values from -0.046875 to 0.046875
- up_weight: bfloat16 [16384, 26624], P('col', 'row'), may hold values from -0.046875 to 0.046875
Outputs:
- hidden: bfloat16 [256, 26624], P(None, 'row')
The draws below stay inside these ranges and needn't reach their ends.
All inputs are finite; a program needn't handle non-finite values.
Results may differ from the reference program's by a relative error of at most 0.001.
Values may be sent and summed in bfloat16 or wider, within the bound.
No kernel may reach another device: no remote copies, remote signals or barrier semaphores. Data moves between devices by JAX's collectives and lax.ppermute only.
A program may use at most 64 MiB of HBM per device.

```python
import jax
import jax.numpy as jnp
from jax import lax

D = 16384
FF = 26624
TOKENS = 256
N_COL = 32


def strengthened(result, rng, source, target, parts, factor):
    owner, partner = [(jnp.arange(result.shape[axis_at]) // (result.shape[axis_at] // parts)).reshape([-1 if axis == axis_at else 1 for axis in range(result.ndim)]) for axis_at in (source, target)]
    chosen = jax.random.permutation(rng, parts)[partner]
    strong = (owner == chosen) | (owner == (partner + parts // 2) % parts)
    return jnp.where(strong, factor * result, result)


def level_of(key, extent, shards, least, largest):
    gain, own = 1.0, jax.random.fold_in(key, 6)
    for dim, blocks in shards:
        heights = jnp.exp(jax.random.uniform(jax.random.fold_in(own, dim), (blocks,), jnp.float32, least / len(shards), largest / len(shards)))
        gain = gain * jnp.repeat(heights, extent[dim] // blocks).reshape([-1 if axis == dim else 1 for axis in range(len(extent))])
    return gain


def noise(key, shape, width, limit, pieces=(), held_as=jnp.bfloat16):
    loudness = level_of(key, shape, pieces, -0.22, 0.18) if pieces else 1.0
    drawn = jax.random.normal(key, shape, jnp.float32) * width * loudness
    return jnp.minimum(jnp.maximum(drawn, -limit), limit).astype(held_as)


def heavy_noise(key, extent, scale, reach, split, heavy, kind=jnp.bfloat16):
    entries = scale * jax.random.normal(key, extent, jnp.float32)
    if split:
        entries = entries * level_of(key, extent, split, -0.22, 0.18)
    return jnp.clip(strengthened(entries, jax.random.fold_in(key, 3), *heavy), -reach, reach).astype(kind)


def setup_inputs(seed: int = 0) -> dict:
    arg_keys = jax.random.split(jax.random.key(seed), 4)
    return {
        "tokens": heavy_noise(arg_keys[0], (TOKENS, D), 1.0, 6.0, ((0, 16), (1, 32)), (1, 0, 32, 2.75)),
        "gate_weight": noise(arg_keys[1], (D, FF), D ** -0.5, 0.046875, ((0, 32), (1, 16))),
        "up_weight": noise(arg_keys[2], (D, FF), D ** -0.5, 0.046875, ((0, 32), (1, 16))),
    }


def reference(tokens, gate_weight, up_weight):
    stride = D // N_COL

    def accumulate(totals, index):
        offset = (index * stride).astype(jnp.int32)
        feature_cols = lax.dynamic_slice_in_dim(tokens, offset, stride, 1)
        gate_block = lax.dynamic_slice_in_dim(gate_weight, offset, stride, 0)
        up_block = lax.dynamic_slice_in_dim(up_weight, offset, stride, 0)
        gate_part = jnp.dot(feature_cols, gate_block, preferred_element_type=jnp.float32)
        up_part = jnp.dot(feature_cols, up_block, preferred_element_type=jnp.float32)
        return (totals[0] + gate_part, totals[1] + up_part), None

    zeros = jnp.zeros((TOKENS, FF), jnp.float32)
    (gate, up), _ = lax.scan(accumulate, (zeros, zeros), jnp.arange(N_COL, dtype=jnp.int32))
    return (jax.nn.silu(gate) * up).astype(jnp.bfloat16)
```

```python
import jax
import jax.numpy as jnp
from jax import lax
from jax.sharding import Mesh
from jax.sharding import PartitionSpec as P

ROW = "row"
FAR = "z_far"
NEAR = ("z_near", "x_lo")
LANES = 128
HALF_RANGE = 125.0


def copy_for_each(value, axis):
    devices = lax.axis_size(axis)
    return lax.all_to_all(
        jnp.broadcast_to(value[None], (devices, *value.shape)), axis, 0, 0, tiled=True
    )


def gathered(value, axis):
    pieces = copy_for_each(value, axis)
    return pieces.reshape(pieces.shape[0] * pieces.shape[1], *pieces.shape[2:])


def coded(rows):
    largest = jnp.max(jnp.abs(rows), axis=-1, keepdims=True)
    largest = jnp.maximum(largest * (1.0 + 2.0**-6), 1e-30).astype(jnp.bfloat16)
    scale = (2.0 * HALF_RANGE) / largest.astype(jnp.float32)
    power = jnp.exp2(jnp.abs(rows) * scale - HALF_RANGE)
    code = jnp.where(rows < 0, -power, power).astype(jnp.bfloat16)
    return jnp.concatenate(
        [code, jnp.broadcast_to(largest, (*largest.shape[:-1], LANES))], axis=-1
    )


def decoded(message):
    code = message[..., :-LANES].astype(jnp.float32)
    largest = message[..., -LANES:][..., :1].astype(jnp.float32)
    size = (jnp.log2(jnp.abs(code)) + HALF_RANGE) * (largest / (2.0 * HALF_RANGE))
    return jnp.where(code < 0, -size, size)


def summed_rows(value, axis):
    devices = lax.axis_size(axis)
    message = coded(value)
    pieces = lax.all_to_all(
        message.reshape(devices, message.shape[0] // devices, message.shape[1]), axis, 0, 0, tiled=True
    )
    return jnp.sum(decoded(pieces), axis=0)


def local(tokens, gate_weight, up_weight):
    columns = gate_weight.shape[1]
    block_rows = gathered(tokens, ROW)
    gate_term = jnp.dot(block_rows, gate_weight, preferred_element_type=jnp.float32)
    up_term = jnp.dot(block_rows, up_weight, preferred_element_type=jnp.float32)
    partial_value = jnp.concatenate([gate_term, up_term], axis=1)
    total = summed_rows(summed_rows(partial_value, NEAR), FAR)
    gated = (jax.nn.silu(total[:, :columns]) * total[:, columns:]).astype(jnp.bfloat16)
    return gathered(gathered(gated, FAR), NEAR)


def solution(mesh):
    split = Mesh(
        mesh.devices.reshape(mesh.shape["row"], 8, 2, 2), ("row", "z_far", "z_near", "x_lo")
    )
    col = ("z_far", "z_near", "x_lo")
    return jax.shard_map(
        local,
        mesh=split,
        in_specs=(P("row", col), P(col, "row"), P(col, "row")),
        out_specs=P(None, "row"),
        check_vma=False,
    )
```

```python
import functools

import jax
import jax.numpy as jnp
from jax import lax
from jax.experimental import pallas as pl
from jax.experimental.pallas import tpu as pltpu
from jax.sharding import Mesh
from jax.sharding import PartitionSpec as P

ROW = "row"
COL = ("z_4", "z_2", "z_1", "x_lo")
FAR = ("z_4", "z_2")
NEAR = ("z_1", "x_lo")
LANES = 128
ROWS = 8
HALF_RANGE = 125.0
STEPS = ((0, 1), (1, 1), (-1, 1), (2, 1), (1, 0), (-1, 0), (-2, 0))


def copy_for_each(value, axis):
    devices = lax.axis_size(axis)
    return lax.all_to_all(
        jnp.broadcast_to(value[None], (devices, *value.shape)), axis, 0, 0, tiled=True
    )


def gathered(value, axis):
    pieces = copy_for_each(value, axis)
    return pieces.reshape(pieces.shape[0] * pieces.shape[1], *pieces.shape[2:])


def largest_of(tiles):
    peak = functools.reduce(jnp.maximum, [jnp.abs(tile) for tile in tiles])
    peak = jnp.max(peak, axis=-1, keepdims=True)
    return jnp.maximum(peak * (1.0 + 2.0**-6), 1e-30).astype(jnp.bfloat16)


def coded(tile, scale):
    power = jnp.exp2(jnp.abs(tile) * scale - HALF_RANGE)
    return jnp.where(tile < 0, -power, power)


def decoded(code, unit):
    code = code.astype(jnp.float32)
    size = (jnp.log2(jnp.abs(code)) + HALF_RANGE) * unit
    return jnp.where(code < 0, -size, size)


def lanes_of(tile):
    return pl.ds(tile * LANES, LANES)


def write_message(values, starts, message, first_row, tiles):
    blocks = [[values[pl.ds(start, ROWS), lanes_of(t)] for t in range(tiles)] for start in starts]
    largest = [largest_of(block) for block in blocks]
    scales = [(2.0 * HALF_RANGE) / peak.astype(jnp.float32) for peak in largest]
    rows = pl.ds(first_row, ROWS * len(starts))
    for t in range(tiles):
        codes = [coded(block[t], scale) for block, scale in zip(blocks, scales)]
        message[rows, lanes_of(t)] = jnp.concatenate(codes, axis=0).astype(jnp.bfloat16)
    marks = [jnp.broadcast_to(peak.astype(jnp.float32), (ROWS, LANES)) for peak in largest]
    message[rows, lanes_of(tiles)] = jnp.concatenate(marks, axis=0).astype(jnp.bfloat16)


def first_body(place, tokens, gate_weight, up_weight, *refs):
    *messages, own, values = refs
    columns = gate_weight.shape[1]
    rows = tokens[...]
    values[:, :columns] = jnp.dot(rows, gate_weight[...], preferred_element_type=jnp.float32)
    values[:, columns:] = jnp.dot(rows, up_weight[...], preferred_element_type=jnp.float32)
    tiles = 2 * columns // LANES
    z, x = place[0], place[1]

    def start_of(step_z, step_x, far):
        owner = (z + step_z + 4) % 4
        near = (owner % 2) * 2 + (x + step_x) % 2
        return pl.multiple_of((near * 8 + far * 2 + owner // 2) * ROWS, ROWS)

    for (step_z, step_x), message in zip(STEPS, messages):
        for far in (0, 2):
            starts = [start_of(step_z, step_x, far + i) for i in range(2)]
            write_message(values, starts, message, far * ROWS, tiles)
    for far in range(4):
        own[pl.ds(far * ROWS, ROWS), :] = values[pl.ds(start_of(0, 0, far), ROWS), :]


def second_body(*refs):
    own, *messages = refs[:-2]
    out, values = refs[-2:]
    tiles = own.shape[1] // LANES
    for half in range(own.shape[0] // 16):
        rows = pl.ds(half * 16, 16)
        units = [m[rows, lanes_of(tiles)].astype(jnp.float32) * (0.5 / HALF_RANGE) for m in messages]
        for t in range(tiles):
            total = own[rows, lanes_of(t)]
            for message, unit in zip(messages, units):
                total = total + decoded(message[rows, lanes_of(t)], unit)
            values[rows, lanes_of(t)] = total
    for far in range(out.shape[0]):
        write_message(values, [far * ROWS], out.at[far], 0, tiles)


def third_body(message, out):
    devices, _, width = message.shape
    tiles = width // LANES - 1
    units = [message[d, :, lanes_of(tiles)].astype(jnp.float32) * (0.5 / HALF_RANGE) for d in range(devices)]

    def total(t):
        return sum(decoded(message[d, :, lanes_of(t)], units[d]) for d in range(devices))

    for t in range(tiles // 2):
        gate, up = total(t), total(t + tiles // 2)
        hidden = (gate * (1.0 / (1.0 + jnp.exp(-gate))) * up).astype(jnp.bfloat16)
        for d in range(out.shape[0]):
            out[d, :, lanes_of(t)] = hidden


def vmem(count):
    return [pl.BlockSpec(memory_space=pltpu.VMEM)] * count


def local(tokens, gate_weight, up_weight):
    columns = gate_weight.shape[1]
    width = 2 * columns + LANES
    block_rows = gathered(tokens, ROW)
    place = jnp.stack(
        [lax.axis_index("z_2") * 2 + lax.axis_index("z_1"), lax.axis_index("x_lo")]
    ).astype(jnp.int32)
    part = block_rows.shape[0] // 8
    f32, bf16 = jnp.float32, jnp.bfloat16
    *messages, own = pl.pallas_call(
        first_body,
        in_specs=[pl.BlockSpec(memory_space=pltpu.SMEM), *vmem(3)],
        out_specs=vmem(len(STEPS) + 1),
        out_shape=[jax.ShapeDtypeStruct((part, width), bf16)] * len(STEPS)
        + [jax.ShapeDtypeStruct((part, 2 * columns), f32)],
        scratch_shapes=[pltpu.VMEM((block_rows.shape[0], 2 * columns), f32)],
    )(place, block_rows, gate_weight, up_weight)
    arrived = []
    for (step_z, step_x), message in zip(STEPS, messages):
        pairs = [
            (z * 2 + x, (z + step_z) % 16 * 2 + (x + step_x) % 2) for z in range(16) for x in range(2)
        ]
        arrived.append(lax.ppermute(message, COL, pairs))
    summed = pl.pallas_call(
        second_body,
        in_specs=vmem(len(STEPS) + 1),
        out_specs=vmem(1)[0],
        out_shape=jax.ShapeDtypeStruct((4, ROWS, width), bf16),
        scratch_shapes=[pltpu.VMEM((part, 2 * columns), f32)],
    )(own, *arrived)
    summed = lax.all_to_all(summed, "z_4", 0, 0, tiled=True)
    copies = pl.pallas_call(
        third_body,
        in_specs=vmem(1),
        out_specs=vmem(1)[0],
        out_shape=jax.ShapeDtypeStruct((8, ROWS, columns), bf16),
    )(summed)
    far = lax.all_to_all(copies, FAR, 0, 0, tiled=True).reshape(64, columns)
    return gathered(far, NEAR)


def solution(mesh):
    split = Mesh(mesh.devices.reshape(mesh.shape["row"], 4, 2, 2, 2), ("row", *COL))
    return jax.shard_map(
        local,
        mesh=split,
        in_specs=(P("row", COL), P(COL, "row"), P(COL, "row")),
        out_specs=P(None, "row"),
        check_vma=False,
    )
```

```python
import functools

import jax
import jax.numpy as jnp
from jax import lax
from jax.experimental import pallas as pl
from jax.experimental.pallas import tpu as pltpu
from jax.sharding import Mesh
from jax.sharding import PartitionSpec as P

ROW = "row"
FAR = "z_far"
NEAR = ("z_near", "x_lo")
COL = (FAR, *NEAR)
LANES = 128
ROWS = 8
HALF_RANGE = 125.0


def copy_for_each(value, axis):
    devices = lax.axis_size(axis)
    return lax.all_to_all(
        jnp.broadcast_to(value[None], (devices, *value.shape)), axis, 0, 0, tiled=True
    )


def gathered(value, axis):
    pieces = copy_for_each(value, axis)
    return pieces.reshape(pieces.shape[0] * pieces.shape[1], *pieces.shape[2:])


def largest_of(tiles):
    peak = functools.reduce(jnp.maximum, [jnp.abs(tile) for tile in tiles])
    peak = jnp.max(peak, axis=-1, keepdims=True)
    return jnp.maximum(peak * (1.0 + 2.0**-6), 1e-30).astype(jnp.bfloat16).astype(jnp.float32)


def coded(tile, scale):
    power = jnp.exp2(jnp.abs(tile) * scale - HALF_RANGE)
    return jnp.where(tile < 0, -power, power)


def decoded(code, unit):
    code = code.astype(jnp.float32)
    size = (jnp.log2(jnp.abs(code)) + HALF_RANGE) * unit
    return jnp.where(code < 0, -size, size)


def lanes_of(tile):
    return pl.ds(tile * LANES, LANES)


def write_rows(values, message):
    tiles = [values[:, lanes_of(t)] for t in range(values.shape[1] // LANES)]
    largest = largest_of(tiles)
    scale = (2.0 * HALF_RANGE) / largest
    for t, tile in enumerate(tiles):
        message[:, lanes_of(t)] = coded(tile, scale).astype(jnp.bfloat16)
    mark = jnp.broadcast_to(largest, (largest.shape[0], LANES))
    message[:, lanes_of(len(tiles))] = mark.astype(jnp.bfloat16)


def sum_of(message, rows, tile, units):
    return sum(decoded(message[d, rows, lanes_of(tile)], unit) for d, unit in enumerate(units))


def units_of(message, rows):
    last = message.shape[2] // LANES - 1
    return [
        message[d, rows, lanes_of(last)].astype(jnp.float32) * (0.5 / HALF_RANGE)
        for d in range(message.shape[0])
    ]


def first_body(tokens, gate_weight, up_weight, message, values, held, arrivals):
    columns = gate_weight.shape[1]
    copies = [
        pltpu.make_async_copy(weight, held.at[i], arrivals.at[i])
        for i, weight in enumerate((gate_weight, up_weight))
    ]
    for copy in copies:
        copy.start()
    for i, copy in enumerate(copies):
        copy.wait()
        values[:, i * columns : (i + 1) * columns] = jnp.dot(
            tokens[...], held[i], preferred_element_type=jnp.float32
        )
    for block in range(message.shape[0]):
        @pl.loop(0, message.shape[1], step=2 * ROWS)
        def _(start):
            start = pl.multiple_of(start, 2 * ROWS)
            write_rows(
                values.at[pl.ds(block * message.shape[1] + start, 2 * ROWS)],
                message.at[block, pl.ds(start, 2 * ROWS)],
            )


def second_body(pieces, message, values):
    @pl.loop(0, pieces.shape[1], step=2 * ROWS)
    def _(start):
        rows = pl.ds(pl.multiple_of(start, 2 * ROWS), 2 * ROWS)
        units = units_of(pieces, rows)
        for t in range(values.shape[1] // LANES):
            values[rows, lanes_of(t)] = sum_of(pieces, rows, t, units)

    @pl.loop(0, message.shape[0])
    def _(far):
        write_rows(values.at[pl.ds(pl.multiple_of(far * ROWS, ROWS), ROWS)], message.at[far])


def third_body(pieces, copies):
    rows = pl.ds(0, pieces.shape[1])
    units = units_of(pieces, rows)
    tiles = copies.shape[2] // LANES
    for t in range(tiles):
        gate, up = sum_of(pieces, rows, t, units), sum_of(pieces, rows, t + tiles, units)
        hidden = (gate / (1.0 + jnp.exp(-gate)) * up).astype(jnp.bfloat16)
        for d in range(copies.shape[0]):
            copies[d, :, lanes_of(t)] = hidden


def on_chip(body, shape, *operands, stored=(), scratch=()):
    on_chip_operands = [pltpu.with_memory_space_constraint(value, pltpu.VMEM) for value in operands]
    return pl.pallas_call(
        body,
        in_specs=[pl.BlockSpec(memory_space=pltpu.VMEM)] * len(operands)
        + [pl.BlockSpec(memory_space=pl.ANY)] * len(stored),
        out_specs=pl.BlockSpec(memory_space=pltpu.VMEM),
        out_shape=pltpu.VMEM(shape, jnp.bfloat16),
        scratch_shapes=scratch,
        compiler_params=pltpu.CompilerParams(vmem_limit_bytes=16 * 2**20),
    )(*on_chip_operands, *stored)


def local(tokens, gate_weight, up_weight):
    columns = gate_weight.shape[1]
    width = 2 * columns + LANES
    block_rows = gathered(tokens, ROW)
    count = block_rows.shape[0]
    near = lax.axis_size(NEAR)
    far = lax.axis_size(FAR)
    coded_parts = on_chip(
        first_body,
        (near, count // near, width),
        block_rows,
        stored=(gate_weight, up_weight),
        scratch=[
            pltpu.VMEM((count, 2 * columns), jnp.float32),
            pltpu.VMEM((2, *gate_weight.shape), jnp.bfloat16),
            pltpu.SemaphoreType.DMA((2,)),
        ],
    )
    near_parts = lax.all_to_all(coded_parts, NEAR, 0, 0, tiled=True)
    coded_sums = on_chip(
        second_body,
        (far, ROWS, width),
        near_parts,
        scratch=[pltpu.VMEM((count // near, 2 * columns), jnp.float32)],
    )
    far_parts = lax.all_to_all(coded_sums, FAR, 0, 0, tiled=True)
    copies = on_chip(third_body, (far, ROWS, columns), far_parts)
    hidden = lax.all_to_all(copies, FAR, 0, 0, tiled=True).reshape(count // near, columns)
    return gathered(hidden, NEAR)


def solution(mesh):
    split = Mesh(mesh.devices.reshape(mesh.shape["row"], 8, 2, 2), (ROW, *COL))
    return jax.shard_map(
        local,
        mesh=split,
        in_specs=(P(ROW, COL), P(COL, ROW), P(COL, ROW)),
        out_specs=P(None, ROW),
        check_vma=False,
    )
```

```python
import functools

import jax
import jax.numpy as jnp
from jax import lax
from jax.experimental import pallas as pl
from jax.experimental.pallas import tpu as pltpu
from jax.sharding import Mesh
from jax.sharding import PartitionSpec as P

ROW = "row"
FAR = "z_4"
COL = ("z_4", "z_2", "z_1", "x_lo")
GATHER_FAR = ("z_4", "z_2")
GATHER_NEAR = ("z_1", "x_lo")
LANES = 128
ROWS = 8
HALF_RANGE = 125.0
STEPS = ((2, 1), (0, 1), (-2, 0), (1, 1), (-1, 1), (1, 0), (-1, 0))
EARLY = 2


def copy_for_each(value, axis):
    devices = lax.axis_size(axis)
    return lax.all_to_all(
        jnp.broadcast_to(value[None], (devices, *value.shape)), axis, 0, 0, tiled=True
    )


def gathered(value, axis):
    pieces = copy_for_each(value, axis)
    return pieces.reshape(pieces.shape[0] * pieces.shape[1], *pieces.shape[2:])


def lanes_of(tile):
    return pl.ds(tile * LANES, LANES)


def largest_of(values, start, tiles):
    peak = functools.reduce(
        jnp.maximum, [jnp.abs(values[pl.ds(start, ROWS), lanes_of(t)]) for t in range(tiles)]
    )
    peak = jnp.max(peak, axis=-1, keepdims=True)
    return jnp.maximum(peak * (1.0 + 2.0**-6), 1e-30).astype(jnp.bfloat16).astype(jnp.float32)


def coded(tile, scale):
    power = jnp.exp2(jnp.abs(tile) * scale - HALF_RANGE)
    return jnp.where(tile < 0, -power, power)


def decoded(code, unit):
    code = code.astype(jnp.float32)
    size = (jnp.log2(jnp.abs(code)) + HALF_RANGE) * unit
    return jnp.where(code < 0, -size, size)


def write_message(values, starts, message, group=2):
    tiles = values.shape[1] // LANES
    largest = [largest_of(values, start, tiles) for start in starts]
    scales = [(2.0 * HALF_RANGE) / peak for peak in largest]
    for first in range(0, len(starts), group):
        chosen = range(first, first + group)
        rows = pl.ds(first * ROWS, group * ROWS)
        for t in range(tiles):
            codes = [coded(values[pl.ds(starts[i], ROWS), lanes_of(t)], scales[i]) for i in chosen]
            message[rows, lanes_of(t)] = jnp.concatenate(codes, axis=0).astype(jnp.bfloat16)
        marks = [jnp.broadcast_to(largest[i], (ROWS, LANES)) for i in chosen]
        message[rows, lanes_of(tiles)] = jnp.concatenate(marks, axis=0).astype(jnp.bfloat16)


def starts_of(step_z, step_x):
    owner = (lax.axis_index("z_2") * 2 + lax.axis_index("z_1") + step_z + 4) % 4
    near = (owner % 2) * 2 + (lax.axis_index("x_lo") + step_x) % 2
    return [pl.multiple_of((near * 8 + far * 2 + owner // 2) * ROWS, ROWS) for far in range(4)]


def product_body(tokens, gate_weight, up_weight, *refs):
    values, *messages, held, arrivals = refs
    columns = gate_weight.shape[1]
    copies = [
        pltpu.make_async_copy(weight, held.at[i], arrivals.at[i])
        for i, weight in enumerate((gate_weight, up_weight))
    ]
    for copy in copies:
        copy.start()
    for i, copy in enumerate(copies):
        copy.wait()
        values[:, i * columns : (i + 1) * columns] = jnp.dot(
            tokens[...], held[i], preferred_element_type=jnp.float32
        )
    for step, message in zip(STEPS[:EARLY], messages):
        write_message(values, starts_of(*step), message)


def code_body(values, *messages):
    for step, message in zip(STEPS[EARLY:], messages):
        write_message(values, starts_of(*step), message)


def sum_body(values, *refs):
    *messages, out, totals = refs
    tiles = totals.shape[1] // LANES
    own = starts_of(0, 0)
    for half in range(2):
        rows = pl.ds(half * 2 * ROWS, 2 * ROWS)
        units = [m[rows, lanes_of(tiles)].astype(jnp.float32) * (0.5 / HALF_RANGE) for m in messages]
        for t in range(tiles):
            total = jnp.concatenate(
                [values[pl.ds(own[half * 2 + i], ROWS), lanes_of(t)] for i in range(2)], axis=0
            )
            for message, unit in zip(messages, units):
                total = total + decoded(message[rows, lanes_of(t)], unit)
            totals[rows, lanes_of(t)] = total
    for far in range(out.shape[0]):
        write_message(totals, [far * ROWS], out.at[far], 1)


def hidden_body(pieces, copies):
    tiles = copies.shape[2] // LANES
    devices = range(pieces.shape[0])
    units = [
        pieces[d, :, lanes_of(2 * tiles)].astype(jnp.float32) * (0.5 / HALF_RANGE) for d in devices
    ]

    def total(t):
        return sum(decoded(pieces[d, :, lanes_of(t)], units[d]) for d in devices)

    for t in range(tiles):
        gate, up = total(t), total(t + tiles)
        hidden = (gate / (1.0 + jnp.exp(-gate)) * up).astype(jnp.bfloat16)
        for d in range(copies.shape[0]):
            copies[d, :, lanes_of(t)] = hidden


def spec(space):
    return pl.BlockSpec(memory_space=space)


def on_chip(body, outputs, operands, stored=(), scratch=()):
    placed = [pltpu.with_memory_space_constraint(value, pltpu.VMEM) for value in operands]
    kept = [pltpu.with_memory_space_constraint(value, pltpu.HBM) for value in stored]
    return pl.pallas_call(
        body,
        in_specs=[spec(pltpu.VMEM)] * len(placed) + [spec(pltpu.HBM)] * len(kept),
        out_specs=[spec(pltpu.VMEM)] * len(outputs),
        out_shape=[pltpu.VMEM(shape, dtype) for shape, dtype in outputs],
        scratch_shapes=scratch,
        compiler_params=pltpu.CompilerParams(vmem_limit_bytes=16 * 2**20),
    )(*placed, *kept)


def sent(message, step_z, step_x):
    z_size, x_size = 16, 2
    pairs = [
        (z * x_size + x, (z + step_z) % z_size * x_size + (x + step_x) % x_size)
        for z in range(z_size)
        for x in range(x_size)
    ]
    return lax.ppermute(message, COL, pairs)


def local(tokens, gate_weight, up_weight):
    columns = gate_weight.shape[1]
    width = 2 * columns + LANES
    f32, bf16 = jnp.float32, jnp.bfloat16
    block_rows = gathered(tokens, ROW)
    count = block_rows.shape[0]
    message = ((count // 8, width), bf16)
    values, *messages = on_chip(
        product_body,
        [((count, 2 * columns), f32)] + [message] * EARLY,
        [block_rows],
        stored=(gate_weight, up_weight),
        scratch=[pltpu.VMEM((2, *gate_weight.shape), bf16), pltpu.SemaphoreType.DMA((2,))],
    )
    messages += on_chip(code_body, [message] * (len(STEPS) - EARLY), [values])
    arrived = [sent(message, *step) for message, step in zip(messages, STEPS)]
    (sums,) = on_chip(
        sum_body,
        [((4, ROWS, width), bf16)],
        [values, *arrived],
        scratch=[pltpu.VMEM((count // 8, 2 * columns), f32)],
    )
    pieces = lax.all_to_all(sums, FAR, 0, 0, tiled=True)
    (copies,) = on_chip(hidden_body, [((8, ROWS, columns), bf16)], [pieces])
    hidden = lax.all_to_all(copies, GATHER_FAR, 0, 0, tiled=True).reshape(8 * ROWS, columns)
    return gathered(hidden, GATHER_NEAR)


def solution(mesh):
    split = Mesh(mesh.devices.reshape(mesh.shape["row"], 4, 2, 2, 2), (ROW, *COL))
    return jax.shard_map(
        local,
        mesh=split,
        in_specs=(P(ROW, COL), P(COL, ROW), P(COL, ROW)),
        out_specs=P(None, ROW),
        check_vma=False,
    )
```

```python
import functools

import jax
import jax.numpy as jnp
from jax import lax
from jax.experimental import pallas as pl
from jax.experimental.pallas import tpu as pltpu
from jax.sharding import Mesh
from jax.sharding import PartitionSpec as P


ROW = "row"
FAR = "z_4"
COL = ("z_4", "z_2", "z_1", "x_lo")
GATHER_FAR = ("z_4", "z_2")
GATHER_NEAR = ("z_1", "x_lo")
LANES = 128
ROWS = 8
HALF_RANGE = 125.0
STEPS = ((True, 1), (True, 0), (False, 1), (False, 0))
EARLY = 2


def copy_for_each(value, axis):
    devices = lax.axis_size(axis)
    return lax.all_to_all(
        jnp.broadcast_to(value[None], (devices, *value.shape)), axis, 0, 0, tiled=True
    )


def gathered(value, axis):
    pieces = copy_for_each(value, axis)
    return pieces.reshape(pieces.shape[0] * pieces.shape[1], *pieces.shape[2:])


def lanes_of(tile):
    return pl.ds(tile * LANES, LANES)


def largest_of(values, start, tiles):
    peak = functools.reduce(
        jnp.maximum, [jnp.abs(values[pl.ds(start, ROWS), lanes_of(t)]) for t in range(tiles)]
    )
    peak = jnp.max(peak, axis=-1, keepdims=True)
    return jnp.maximum(peak * (1.0 + 2.0**-6), 1e-30).astype(jnp.bfloat16).astype(jnp.float32)


def coded(tile, scale):
    power = jnp.exp2(jnp.abs(tile) * scale - HALF_RANGE)
    return jnp.where(tile < 0, -power, power)


def decoded(code, unit):
    code = code.astype(jnp.float32)
    size = (jnp.log2(jnp.abs(code)) + HALF_RANGE) * unit
    return jnp.where(code < 0, -size, size)


def write_message(values, starts, message, group=2):
    tiles = values.shape[1] // LANES
    largest = [largest_of(values, start, tiles) for start in starts]
    scales = [(2.0 * HALF_RANGE) / peak for peak in largest]
    for first in range(0, len(starts), group):
        chosen = range(first, first + group)
        rows = pl.ds(first * ROWS, group * ROWS)
        for t in range(tiles):
            codes = [coded(values[pl.ds(starts[i], ROWS), lanes_of(t)], scales[i]) for i in chosen]
            message[rows, lanes_of(t)] = jnp.concatenate(codes, axis=0).astype(jnp.bfloat16)
        marks = [jnp.broadcast_to(largest[i], (ROWS, LANES)) for i in chosen]
        message[rows, lanes_of(tiles)] = jnp.concatenate(marks, axis=0).astype(jnp.bfloat16)


def starts_of(z_2, z_1, x_lo):
    near = z_1 * 2 + x_lo
    return [pl.multiple_of((near * 8 + far * 2 + z_2) * ROWS, ROWS) for far in range(4)]


def starts_outside(two_away, step_x):
    mine = lax.axis_index("z_1")
    return starts_of(
        1 - lax.axis_index("z_2"),
        mine if two_away else 1 - mine,
        (lax.axis_index("x_lo") + step_x) % 2,
    )


def next_outside(z, two_away):
    direction = 1 - 2 * (z % 2)
    return (z + (2 * direction if two_away else -direction)) % 16


def product_body(tokens, gate_weight, up_weight, *refs):
    values, *messages, held, arrivals = refs
    columns = gate_weight.shape[1]
    copies = [
        pltpu.make_async_copy(weight, held.at[i], arrivals.at[i])
        for i, weight in enumerate((gate_weight, up_weight))
    ]
    for copy in copies:
        copy.start()
    for i, copy in enumerate(copies):
        copy.wait()
        values[:, i * columns : (i + 1) * columns] = jnp.dot(
            tokens[...], held[i], preferred_element_type=jnp.float32
        )
    for step, message in zip(STEPS[:EARLY], messages):
        write_message(values, starts_outside(*step), message)


def code_body(values, pair, *messages):
    for owner in range(pair.shape[0]):
        starts = starts_of(lax.axis_index("z_2"), owner // 2, owner % 2)
        write_message(values, starts, pair.at[owner])
    for step, message in zip(STEPS[EARLY:], messages):
        write_message(values, starts_outside(*step), message)


def sum_body(pair, *refs):
    *messages, out, totals = refs
    messages = [pair.at[i] for i in range(pair.shape[0])] + messages
    tiles = totals.shape[1] // LANES
    for half in range(2):
        rows = pl.ds(half * 2 * ROWS, 2 * ROWS)
        units = [m[rows, lanes_of(tiles)].astype(jnp.float32) * (0.5 / HALF_RANGE) for m in messages]
        for t in range(tiles):
            totals[rows, lanes_of(t)] = sum(
                decoded(message[rows, lanes_of(t)], unit) for message, unit in zip(messages, units)
            )
    for far in range(out.shape[0]):
        write_message(totals, [far * ROWS], out.at[far], 1)


def hidden_body(pieces, copies):
    tiles = copies.shape[2] // LANES
    devices = range(pieces.shape[0])
    units = [
        pieces[d, :, lanes_of(2 * tiles)].astype(jnp.float32) * (0.5 / HALF_RANGE) for d in devices
    ]

    def total(t):
        return sum(decoded(pieces[d, :, lanes_of(t)], units[d]) for d in devices)

    for t in range(tiles):
        gate, up = total(t), total(t + tiles)
        hidden = (gate / (1.0 + jnp.exp(-gate)) * up).astype(jnp.bfloat16)
        for d in range(copies.shape[0]):
            copies[d, :, lanes_of(t)] = hidden


def spec(space):
    return pl.BlockSpec(memory_space=space)


def on_chip(body, outputs, operands, stored=(), scratch=()):
    placed = [pltpu.with_memory_space_constraint(value, pltpu.VMEM) for value in operands]
    kept = [pltpu.with_memory_space_constraint(value, pltpu.HBM) for value in stored]
    return pl.pallas_call(
        body,
        in_specs=[spec(pltpu.VMEM)] * len(placed) + [spec(pltpu.HBM)] * len(kept),
        out_specs=[spec(pltpu.VMEM)] * len(outputs),
        out_shape=[pltpu.VMEM(shape, dtype) for shape, dtype in outputs],
        scratch_shapes=scratch,
        compiler_params=pltpu.CompilerParams(vmem_limit_bytes=16 * 2**20),
    )(*placed, *kept)


def sent(message, two_away, step_x):
    pairs = [
        (z * 2 + x, next_outside(z, two_away) * 2 + (x + step_x) % 2) for z in range(16) for x in range(2)
    ]
    return lax.ppermute(message, COL, pairs)


def layer(tokens, gate_weight, up_weight):
    columns = gate_weight.shape[1]
    width = 2 * columns + LANES
    f32, bf16 = jnp.float32, jnp.bfloat16
    block_rows = gathered(tokens, ROW)
    count = block_rows.shape[0]
    message = ((count // 8, width), bf16)
    values, *messages = on_chip(
        product_body,
        [((count, 2 * columns), f32)] + [message] * EARLY,
        [block_rows],
        stored=(gate_weight, up_weight),
        scratch=[pltpu.VMEM((2, *gate_weight.shape), bf16), pltpu.SemaphoreType.DMA((2,))],
    )
    pair, *others = on_chip(
        code_body,
        [((4, count // 8, width), bf16)] + [message] * (len(STEPS) - EARLY),
        [values],
    )
    arrived = []
    for message, step in zip(messages + others, STEPS):
        arrived.append(sent(message, *step))
    pair = lax.all_to_all(pair, GATHER_NEAR, 0, 0, tiled=True)
    (sums,) = on_chip(
        sum_body,
        [((4, ROWS, width), bf16)],
        [pair, *arrived],
        scratch=[pltpu.VMEM((count // 8, 2 * columns), f32)],
    )
    pieces = lax.all_to_all(sums, FAR, 0, 0, tiled=True)
    (copies,) = on_chip(hidden_body, [((8, ROWS, columns), bf16)], [pieces])
    hidden = lax.all_to_all(copies, GATHER_FAR, 0, 0, tiled=True).reshape(8 * ROWS, columns)
    return gathered(hidden, GATHER_NEAR)


def solution(mesh):
    split = Mesh(mesh.devices.reshape(mesh.shape["row"], 4, 2, 2, 2), (ROW, *COL))
    return jax.shard_map(
        layer,
        mesh=split,
        in_specs=(P(ROW, COL), P(COL, ROW), P(COL, ROW)),
        out_specs=P(None, ROW),
        check_vma=False,
    )
```

```python
import functools

import jax
import jax.numpy as jnp
from jax import lax
from jax.experimental import pallas as pl
from jax.experimental.pallas import tpu as pltpu
from jax.sharding import Mesh
from jax.sharding import PartitionSpec as P


ROW = "row"
FAR = "z_4"
COL = ("z_4", "z_2", "z_1", "x_lo")
GATHER_FAR = ("z_4", "z_2")
GATHER_NEAR = ("z_1", "x_lo")
LANES = 128
ROWS = 8
HALF_RANGE = 125.0
STEPS = ((True, 1), (False, 1), (False, 0), (True, 0))
EARLY = 2


def copy_for_each(value, axis):
    devices = lax.axis_size(axis)
    return lax.all_to_all(
        jnp.broadcast_to(value[None], (devices, *value.shape)), axis, 0, 0, tiled=True
    )


def gathered(value, axis):
    pieces = copy_for_each(value, axis)
    return pieces.reshape(pieces.shape[0] * pieces.shape[1], *pieces.shape[2:])


def lanes_of(tile):
    return pl.ds(tile * LANES, LANES)


def largest_of(values, start, tiles):
    peak = functools.reduce(
        jnp.maximum, [jnp.abs(values[pl.ds(start, ROWS), lanes_of(t)]) for t in range(tiles)]
    )
    peak = jnp.max(peak, axis=-1, keepdims=True)
    return jnp.maximum(peak * (1.0 + 2.0**-6), 1e-30).astype(jnp.bfloat16).astype(jnp.float32)


def coded(tile, scale):
    power = jnp.exp2(jnp.abs(tile) * scale - HALF_RANGE)
    return jnp.where(tile < 0, -power, power)


def decoded(code, unit):
    code = code.astype(jnp.float32)
    size = (jnp.log2(jnp.abs(code)) + HALF_RANGE) * unit
    return jnp.where(code < 0, -size, size)


def write_message(values, starts, message, group=2):
    tiles = values.shape[1] // LANES
    largest = [largest_of(values, start, tiles) for start in starts]
    scales = [(2.0 * HALF_RANGE) / peak for peak in largest]
    for first in range(0, len(starts), group):
        chosen = range(first, first + group)
        rows = pl.ds(first * ROWS, group * ROWS)
        for t in range(tiles):
            codes = [coded(values[pl.ds(starts[i], ROWS), lanes_of(t)], scales[i]) for i in chosen]
            message[rows, lanes_of(t)] = jnp.concatenate(codes, axis=0).astype(jnp.bfloat16)
        marks = [jnp.broadcast_to(largest[i], (ROWS, LANES)) for i in chosen]
        message[rows, lanes_of(tiles)] = jnp.concatenate(marks, axis=0).astype(jnp.bfloat16)


def starts_of(z_2, z_1, x_lo):
    near = z_1 * 2 + x_lo
    return [pl.multiple_of((near * 8 + far * 2 + z_2) * ROWS, ROWS) for far in range(4)]


def starts_outside(two_away, step_x):
    mine = lax.axis_index("z_1")
    return starts_of(
        1 - lax.axis_index("z_2"),
        mine if two_away else 1 - mine,
        (lax.axis_index("x_lo") + step_x) % 2,
    )


def next_outside(z, two_away):
    direction = 1 - 2 * (z % 2)
    return (z + (2 * direction if two_away else -direction)) % 16


def product_body(tokens, gate_weight, up_weight, *refs):
    values, *messages, held, arrivals = refs
    columns = gate_weight.shape[1]
    copies = [
        pltpu.make_async_copy(weight, held.at[i], arrivals.at[i])
        for i, weight in enumerate((gate_weight, up_weight))
    ]
    for copy in copies:
        copy.start()
    for i, copy in enumerate(copies):
        copy.wait()
        values[:, i * columns : (i + 1) * columns] = jnp.dot(
            tokens[...], held[i], preferred_element_type=jnp.float32
        )
    for step, message in zip(STEPS[:EARLY], messages):
        write_message(values, starts_outside(*step), message)


def place_in_pair():
    return lax.axis_index("z_1") * 2 + lax.axis_index("x_lo")


def code_body(values, pair, own, *messages):
    mine, z_2 = place_in_pair(), lax.axis_index("z_2")
    pair[mine] = jnp.zeros(pair.shape[1:], pair.dtype)
    for step in range(1, pair.shape[0]):
        owner = (mine + step) % 4
        write_message(values, starts_of(z_2, owner // 2, owner % 2), pair.at[owner])
    for far, start in enumerate(starts_of(z_2, mine // 2, mine % 2)):
        own[pl.ds(far * ROWS, ROWS), :] = values[pl.ds(start, ROWS), :]
    for step, message in zip(STEPS[EARLY:], messages):
        write_message(values, starts_outside(*step), message)


def units_of(messages, rows):
    return [m[rows, lanes_of(m.shape[1] // LANES - 1)].astype(jnp.float32) * (0.5 / HALF_RANGE) for m in messages]


def add_decoded(first, messages, totals):
    for half in range(2):
        rows = pl.ds(half * 2 * ROWS, 2 * ROWS)
        units = units_of(messages, rows)
        for t in range(totals.shape[1] // LANES):
            total = first[rows, lanes_of(t)]
            for message, unit in zip(messages, units):
                total = total + decoded(message[rows, lanes_of(t)], unit)
            totals[rows, lanes_of(t)] = total


def early_sum_body(own, *refs):
    *messages, totals = refs
    add_decoded(own, messages, totals)


def sum_body(early, pair, *refs):
    *messages, out, totals = refs
    mine = place_in_pair()
    others = [pair.at[(mine + step) % 4] for step in range(1, pair.shape[0])]
    add_decoded(early, others + messages, totals)
    for far in range(out.shape[0]):
        write_message(totals, [far * ROWS], out.at[far], 1)


def hidden_body(pieces, copies):
    tiles = copies.shape[2] // LANES
    devices = range(pieces.shape[0])
    units = [
        pieces[d, :, lanes_of(2 * tiles)].astype(jnp.float32) * (0.5 / HALF_RANGE) for d in devices
    ]

    def total(t):
        return sum(decoded(pieces[d, :, lanes_of(t)], units[d]) for d in devices)

    for t in range(tiles):
        gate, up = total(t), total(t + tiles)
        hidden = (gate / (1.0 + jnp.exp(-gate)) * up).astype(jnp.bfloat16)
        for d in range(copies.shape[0]):
            copies[d, :, lanes_of(t)] = hidden


def spec(space):
    return pl.BlockSpec(memory_space=space)


def on_chip(body, outputs, operands, stored=(), scratch=()):
    placed = [pltpu.with_memory_space_constraint(value, pltpu.VMEM) for value in operands]
    kept = [pltpu.with_memory_space_constraint(value, pltpu.HBM) for value in stored]
    return pl.pallas_call(
        body,
        in_specs=[spec(pltpu.VMEM)] * len(placed) + [spec(pltpu.HBM)] * len(kept),
        out_specs=[spec(pltpu.VMEM)] * len(outputs),
        out_shape=[pltpu.VMEM(shape, dtype) for shape, dtype in outputs],
        scratch_shapes=scratch,
        compiler_params=pltpu.CompilerParams(vmem_limit_bytes=16 * 2**20),
    )(*placed, *kept)


def sent(message, two_away, step_x):
    pairs = [
        (z * 2 + x, next_outside(z, two_away) * 2 + (x + step_x) % 2) for z in range(16) for x in range(2)
    ]
    return lax.ppermute(message, COL, pairs)


def layer(tokens, gate_weight, up_weight):
    columns = gate_weight.shape[1]
    width = 2 * columns + LANES
    f32, bf16 = jnp.float32, jnp.bfloat16
    block_rows = gathered(tokens, ROW)
    count = block_rows.shape[0]
    message = ((count // 8, width), bf16)
    values, *messages = on_chip(
        product_body,
        [((count, 2 * columns), f32)] + [message] * EARLY,
        [block_rows],
        stored=(gate_weight, up_weight),
        scratch=[pltpu.VMEM((2, *gate_weight.shape), bf16), pltpu.SemaphoreType.DMA((2,))],
    )
    pair, own, *others = on_chip(
        code_body,
        [((4, count // 8, width), bf16), ((count // 8, 2 * columns), f32)]
        + [message] * (len(STEPS) - EARLY),
        [values],
    )
    arrived = []
    for message, step in zip(messages + others, STEPS):
        arrived.append(sent(message, *step))
    pair = lax.all_to_all(pair, GATHER_NEAR, 0, 0, tiled=True)
    (early,) = on_chip(early_sum_body, [((count // 8, 2 * columns), f32)], [own, *arrived[:EARLY]])
    (sums,) = on_chip(
        sum_body,
        [((4, ROWS, width), bf16)],
        [early, pair, *arrived[EARLY:]],
        scratch=[pltpu.VMEM((count // 8, 2 * columns), f32)],
    )
    pieces = lax.all_to_all(sums, FAR, 0, 0, tiled=True)
    (copies,) = on_chip(hidden_body, [((8, ROWS, columns), bf16)], [pieces])
    hidden = lax.all_to_all(copies, GATHER_FAR, 0, 0, tiled=True).reshape(8 * ROWS, columns)
    return gathered(hidden, GATHER_NEAR)


def solution(mesh):
    split = Mesh(mesh.devices.reshape(mesh.shape["row"], 4, 2, 2, 2), (ROW, *COL))
    return jax.shard_map(
        layer,
        mesh=split,
        in_specs=(P(ROW, COL), P(COL, ROW), P(COL, ROW)),
        out_specs=P(None, ROW),
        check_vma=False,
    )
```
